32 devices in a mesh: prow: 4 (over y, core), pcol: 8 (over z, x).
Axes of the slice: x: 2, y: 2, z: 4, core: 2. Of those that a mesh axis runs over, the one named last changes fastest.
Arguments:
- matrix: bfloat16 [2, 8, 4, 256, 2, 8, 256], P(None, None, 'prow', None, None, 'pcol'), may hold values from -6 to 6
Outputs:
- image: float32 [2, 8, 4, 256, 2, 8, 256], P(None, None, 'prow', None, None, 'pcol')
The draws below stay inside these ranges and needn't reach their ends.
All inputs are finite; a program needn't handle non-finite values.
Results may differ from the reference program's by a relative error of at most 0.0003.
Values sent between devices are 32-bit elements; how exact they have to be, the bound alone decides.
A program may use at most 64 MiB of HBM per device.

```python
import jax
import jax.numpy as jnp

IMAGES = 2
BLOCK = 256
ROW_BLOCKS = 8
COL_BLOCKS = 2
N_PROW = 4
N_PCOL = 8


def block_levels(key, extent, shards, low, high):
    loudness, own = 1.0, jax.random.fold_in(key, 6)
    for position, parts in shards:
        heights = jnp.exp(jax.random.uniform(jax.random.fold_in(own, position), (parts,), jnp.float32, low / len(shards), high / len(shards)))
        loudness = loudness * jnp.repeat(heights, extent[position] // parts).reshape([-1 if axis == position else 1 for axis in range(len(extent))])
    return loudness


def normal_values(stream_key, extent, spread, bound, split=(), kind=jnp.bfloat16):
    factor_of = block_levels(stream_key, extent, split, -0.22, 0.18) if split else 1.0
    result = jax.random.normal(stream_key, extent, jnp.float32) * spread * factor_of
    return jnp.minimum(jnp.maximum(result, -bound), bound).astype(kind)


def setup_inputs(seed: int = 0) -> dict:
    arg_keys = jax.random.split(jax.random.key(seed), 2)
    matrix = normal_values(arg_keys[0], (IMAGES, ROW_BLOCKS, N_PROW, BLOCK, COL_BLOCKS, N_PCOL, BLOCK), 1.0, 6.0, ((2, 4), (5, 8)))
    return {"matrix": matrix}


def reference(matrix):
    total_rows = ROW_BLOCKS * N_PROW * BLOCK
    total_cols = COL_BLOCKS * N_PCOL * BLOCK
    full = matrix.astype(jnp.float32).reshape(IMAGES, total_rows, total_cols)
    summed = jnp.cumsum(jnp.cumsum(full, axis=1, dtype=jnp.float32), axis=2, dtype=jnp.float32)
    row_factor = 1.0 / jnp.sqrt(jnp.arange(total_rows).astype(jnp.float32) + 1.0)
    col_factor = 1.0 / jnp.sqrt(jnp.arange(total_cols).astype(jnp.float32) + 1.0)
    scaled = summed * (row_factor[None, :, None] * col_factor[None, None, :])
    return scaled.reshape(IMAGES, ROW_BLOCKS, N_PROW, BLOCK, COL_BLOCKS, N_PCOL, BLOCK)
```

```python
import functools

import jax
import jax.numpy as jnp
from jax import lax
from jax.experimental import pallas as pl
from jax.experimental.pallas import tpu as pltpu
from jax.sharding import PartitionSpec as P

F32, BF16 = jnp.float32, jnp.bfloat16
HIGH = lax.Precision.HIGHEST
MESH = pl.DeviceIdType.MESH
NN = (((1,), (0,)), ((), ()))
SUBS = 8
LANES = 128


def iotas(rows, cols):
    return (lax.broadcasted_iota(jnp.int32, (rows, cols), 0), lax.broadcasted_iota(jnp.int32, (rows, cols), 1))


def local(np_, nq, rows_here, x_hbm, t_ref, c_ref, d_ref, rf_ref, xbuf, up_ref, e_ref, b_ref, k_ref, e_all, b_all, k_all,
          in_sem, e_send, e_recv, b_send, b_recv, k_send, k_recv):
    groups, tile, cols, width = x_hbm.shape
    steps = tile // SUBS
    n = SUBS * cols
    per = LANES // steps
    p, q = lax.axis_index("prow"), lax.axis_index("pcol")
    total = np_ * nq
    me = p * nq + q
    loads = [pltpu.make_async_copy(x_hbm.at[g], xbuf.at[g], in_sem.at[g]) for g in range(groups)]
    for load in loads:
        load.start()

    barrier = pltpu.get_barrier_semaphore()

    def greet(k, _):
        dev = lax.rem(me + k, total)
        pl.semaphore_signal(barrier, inc=1, device_id=(dev // nq, lax.rem(dev, nq)), device_id_type=MESH)
        return 0

    lax.fori_loop(1, total, greet, 0)

    u0, u1 = iotas(width, width)
    up_ref[...] = (u0 <= u1).astype(BF16)
    _, lane = iotas(n, LANES)
    sub, _ = iotas(per * cols, width)

    def block(b, _):
        for k in range(per):
            g = b * per + k
            pltpu.make_async_copy(x_hbm.at[g], xbuf.at[g], in_sem.at[g]).wait()
        e = jnp.zeros((n, LANES), F32)
        bottom = jnp.zeros((per * cols, width), F32)
        for k in range(per):
            g = b * per + k
            x = xbuf[g].reshape(SUBS, steps, cols, width)
            x = jnp.swapaxes(x, 0, 1).reshape(steps * n, width)
            z = lax.dot_general(x, up_ref[...], NN, preferred_element_type=F32)
            acc = jnp.zeros((n, width), F32)
            for i in range(steps):
                acc = acc + z[i * n:(i + 1) * n]
                t_ref[g, pl.ds(i * n, n), :] = acc
                e = jnp.where(lane == k * steps + i, jnp.broadcast_to(acc[:, width - 1:], (n, LANES)), e)
            w = acc[:n // 2] + acc[n // 2:]
            w = w + pltpu.roll(w, cols, 0)
            w = w + pltpu.roll(w, 2 * cols, 0)
            bottom = jnp.where(sub // cols == k, w, bottom)
        e_ref[b] = e
        b_ref[b] = bottom
        return 0

    lax.fori_loop(0, groups // per, block, 0)

    k0, k1 = iotas(per * cols, LANES)
    corner = jnp.zeros((per * cols, LANES), F32)
    for b in range(groups // per):
        edge = jnp.broadcast_to(b_ref[b][:, width - 1:], (per * cols, LANES))
        corner = jnp.where(k1 == b * per * cols + k0, edge, corner)
    k_ref[0] = jnp.sum(corner, axis=0, keepdims=True)
    pl.semaphore_wait(barrier, total - 1)

    def e_copy(k, sender, target):
        return pltpu.make_async_remote_copy(
            src_ref=e_ref, dst_ref=e_all.at[sender], send_sem=e_send.at[k], recv_sem=e_recv.at[sender],
            device_id=(p, target), device_id_type=MESH)

    def b_copy(k, sender, target):
        return pltpu.make_async_remote_copy(
            src_ref=b_ref, dst_ref=b_all.at[sender], send_sem=b_send.at[k], recv_sem=b_recv.at[sender],
            device_id=(target, q), device_id_type=MESH)

    def k_copy(k, sender, target):
        return pltpu.make_async_remote_copy(
            src_ref=k_ref.at[0], dst_ref=k_all.at[sender], send_sem=k_send.at[k], recv_sem=k_recv.at[sender],
            device_id=(target // nq, lax.rem(target, nq)), device_id_type=MESH)

    kinds = ((k_copy, me, total), (b_copy, p, np_), (e_copy, q, nq))
    for make, here, count in kinds:
        def send(k, _):
            make(k, here, lax.rem(here + k, count)).start()
            return 0
        lax.fori_loop(1, count, send, 0)

    def drain(make, here, count):
        def wait(k, _):
            make(k, lax.rem(here + k, count), lax.rem(here + k, count)).wait_recv()
            return 0
        lax.fori_loop(1, count, wait, 0)

    r0, _ = iotas(n, LANES)

    def factors(r, _):
        for i in range(steps):
            row = (r * np_ + p) * tile + (r0 // cols) * steps + i
            rf_ref[r, pl.ds(i * n, n), :] = 1.0 / jnp.sqrt((row + 1).astype(F32))
        return 0

    lax.fori_loop(0, rows_here, factors, 0)

    drain(*kinds[0])
    k_all[pl.ds(me, 1)] = k_ref[...]

    def k_sum(k, acc):
        a_all, a_lt, c_all, c_lt = acc
        value = k_all[k]
        kp, kq = k // nq, lax.rem(k, nq)
        left = jnp.where(kq < q, value, 0.0)
        up = jnp.where(kp < p, value, 0.0)
        both = jnp.where(kp < p, left, 0.0)
        return a_all + left, a_lt + both, c_all + value, c_lt + up

    zero = jnp.zeros((1, LANES), F32)
    a_all, a_lt, c_all, c_lt = lax.fori_loop(0, total, k_sum, (zero,) * 4)
    rows = groups * cols
    out, src = iotas(rows, LANES)
    out_g, src_g = out // cols, src // cols
    out_c, src_c = lax.rem(out, cols), lax.rem(src, cols)
    same_g = out_g == src_g
    above = (out_g // rows_here == src_g // rows_here) & (src_g < out_g)
    weigh = lambda strict, all_rows, lt_rows: (
        jnp.where(above & strict, all_rows, 0.0) + jnp.where(same_g & strict, lt_rows, 0.0))
    corner = jnp.sum(weigh(src_c == out_c, a_all, a_lt) + weigh(src_c < out_c, c_all, c_lt), axis=1, keepdims=True)

    drain(*kinds[1])
    s_all = b_ref[...].reshape(rows, width)
    s_lt = jnp.zeros_like(s_all)
    for k in range(np_):
        value = jnp.where(k == p, 0.0, b_all[k].reshape(rows, width))
        s_all = s_all + value
        s_lt = s_lt + jnp.where(k < p, value, 0.0)
    o, s = iotas(rows, rows)
    strict = ((o // (rows_here * cols) == s // (rows_here * cols)) & (lax.rem(o, cols) == lax.rem(s, cols))
              & (s // cols < o // cols)).astype(F32)
    pre = lax.dot_general(strict, s_all, NN, precision=HIGH, preferred_element_type=F32)
    d_ref[...] = (pre + s_lt + corner).reshape(groups // per, per * cols, width)

    drain(*kinds[2])
    flat = groups // per * n
    r_all = e_ref[...].reshape(flat, LANES)
    r_lt = jnp.zeros_like(r_all)
    for k in range(nq):
        value = jnp.where(k == q, 0.0, e_all[k].reshape(flat, LANES))
        r_all = r_all + value
        r_lt = r_lt + jnp.where(k < q, value, 0.0)
    f0, _ = iotas(flat, LANES)
    for shift in range(1, cols):
        r_lt = r_lt + jnp.where(lax.rem(f0, cols) >= shift, pltpu.roll(r_all, shift, 0), 0.0)
    c_ref[...] = r_lt.reshape(groups // per, n, LANES)

    for make, here, count in kinds:
        def sent(k, _):
            make(k, here, lax.rem(here + k, count)).wait_send()
            return 0
        lax.fori_loop(1, count, sent, 0)


def finish(np_, nq, rows_here, t_ref, c_ref, d_ref, rf_ref, out_hbm, obuf, cb_refs, dp_refs, sem):
    groups, rows, width = t_ref.shape
    cols = out_hbm.shape[3]
    n = SUBS * cols
    steps = rows // n
    per = LANES // steps
    lanes = width // LANES
    q = lax.axis_index("pcol")
    c0, c1 = iotas(n, width)
    cf = 1.0 / jnp.sqrt(((lax.rem(c0, cols) * nq + q) * width + c1 + 1).astype(F32))
    pitch = (steps + 1) * lanes
    sub, _ = iotas(per * cols, width)

    def prepare(g, slot):
        c = pltpu.roll(c_ref[g // per], LANES - lax.rem(g, per) * steps, 1)
        for i in range(steps):
            cb = jnp.broadcast_to(c[:, i:i + 1], (n, LANES))
            cb_refs[slot][pl.ds(i * n, n), :] = cb
        v = t_ref[g, pl.ds((steps - 1) * n, n), :] + jnp.concatenate([cb] * lanes, axis=1)
        v = jnp.where(c0 >= cols, pltpu.roll(v, cols, 0), 0.0)
        shift = cols
        while shift < n:
            v = v + jnp.where(c0 >= shift, pltpu.roll(v, shift, 0), 0.0)
            shift *= 2
        d = jnp.where(sub // cols == lax.rem(g, per), d_ref[g // per], 0.0)
        shift = cols
        while shift < per * cols:
            d = d + pltpu.roll(d, shift, 0)
            shift *= 2
        dp_refs[slot][...] = v + jnp.concatenate([d] * (n // (per * cols)), axis=0)

    def emit(g, slot):
        r = lax.rem(g, rows_here)
        d = dp_refs[slot][...]
        dst = obuf.at[g].reshape(n * (steps + 1) * lanes, LANES)
        for i in range(steps):
            cut = pl.ds(i * n, n)
            cb, v, f = cb_refs[slot][cut, :], t_ref[g, cut, :], rf_ref[r, cut, :]
            for t in range(lanes):
                col = slice(t * LANES, (t + 1) * LANES)
                o = (v[:, col] + (cb + d[:, col])) * (f * cf[:, col])
                for h in range(0, n, 8):
                    dst[pl.ds(h * pitch + i * lanes + t, 8, stride=pitch), :] = o[h:h + 8]

    def copies(g):
        return [pltpu.make_async_copy(obuf.at[g, k, pl.ds(0, steps)], out_hbm.at[g, k // cols, :, k % cols], sem.at[g, k])
                for k in range(n)]

    prepare(0, 0)

    def pair(b, _):
        for slot in range(2):
            g = b * 2 + slot
            prepare(lax.rem(g + 1, groups), 1 - slot)
            emit(g, slot)
            for copy in copies(g):
                copy.start()
        return 0

    lax.fori_loop(0, groups // 2, pair, 0)

    def drain(g, _):
        for copy in copies(g):
            copy.wait()
        return 0

    lax.fori_loop(0, groups, drain, 0)


def solution(mesh):
    np_, nq = mesh.shape["prow"], mesh.shape["pcol"]

    def shards(matrix):
        batch, rows_here, _, tile, cols, _, width = matrix.shape
        groups, lanes = batch * rows_here, width // LANES
        steps, n, total = tile // SUBS, SUBS * cols, np_ * nq
        per = LANES // steps
        blocks = groups // per
        x = pltpu.with_memory_space_constraint(matrix.reshape(groups, tile, cols, width), pltpu.HBM)
        dma = pltpu.SemaphoreType.DMA
        vmem = pl.BlockSpec(memory_space=pltpu.VMEM)
        carried = pl.pallas_call(
            functools.partial(local, np_, nq, rows_here),
            out_shape=(jax.ShapeDtypeStruct((groups, tile * cols, width), F32),
                       jax.ShapeDtypeStruct((blocks, n, LANES), F32),
                       jax.ShapeDtypeStruct((blocks, per * cols, width), F32),
                       jax.ShapeDtypeStruct((rows_here, tile * cols, LANES), F32)),
            in_specs=[pl.BlockSpec(memory_space=pltpu.HBM)],
            out_specs=(vmem,) * 4,
            scratch_shapes=[
                pltpu.VMEM((groups, tile, cols, width), BF16),
                pltpu.VMEM((width, width), BF16),
                pltpu.VMEM((blocks, n, LANES), F32),
                pltpu.VMEM((blocks, per * cols, width), F32),
                pltpu.VMEM((1, 1, LANES), F32),
                pltpu.VMEM((nq, blocks, n, LANES), F32),
                pltpu.VMEM((np_, blocks, per * cols, width), F32),
                pltpu.VMEM((total, 1, LANES), F32),
                dma((groups,)), dma((nq,)), dma((nq,)), dma((np_,)), dma((np_,)), dma((total,)), dma((total,)),
            ],
            compiler_params=pltpu.CompilerParams(
                collective_id=0, has_side_effects=True, vmem_limit_bytes=24 * 2**20),
            name="local",
        )(x)
        out = pl.pallas_call(
            functools.partial(finish, np_, nq, rows_here),
            out_shape=jax.ShapeDtypeStruct((groups, SUBS, steps, cols, lanes, LANES), F32),
            in_specs=[vmem] * 4,
            out_specs=pl.BlockSpec(memory_space=pl.ANY),
            scratch_shapes=[
                pltpu.VMEM((groups, n, steps + 1, lanes, LANES), F32),
                [pltpu.VMEM((tile * cols, LANES), F32)] * 2,
                [pltpu.VMEM((n, width), F32)] * 2,
                dma((groups, n)),
            ],
            compiler_params=pltpu.CompilerParams(vmem_limit_bytes=24 * 2**20),
            name="finish",
        )(*carried)
        return out.reshape(matrix.shape)

    spec = P(None, None, "prow", None, None, "pcol", None)
    return jax.shard_map(shards, mesh=mesh, in_specs=(spec,), out_specs=spec, check_vma=False)
```

```python
import functools

import jax
import jax.numpy as jnp
from jax import lax
from jax.experimental import pallas as pl
from jax.experimental.pallas import tpu as pltpu
from jax.sharding import PartitionSpec as P

F32, BF16 = jnp.float32, jnp.bfloat16
HIGH = lax.Precision.HIGHEST
MESH = pl.DeviceIdType.MESH
NN = (((1,), (0,)), ((), ()))
SUBS = 8
LANES = 128


def iotas(rows, cols):
    return (lax.broadcasted_iota(jnp.int32, (rows, cols), 0), lax.broadcasted_iota(jnp.int32, (rows, cols), 1))


def shifted(v, rows, cols, count):
    v = jnp.where(rows >= cols, pltpu.roll(v, cols, 0), 0.0)
    shift = cols
    while shift < count:
        v = v + jnp.where(rows >= shift, pltpu.roll(v, shift, 0), 0.0)
        shift *= 2
    return v


def local(np_, nq, rows_here, x_hbm, t_ref, pt_ref, c_ref, d_ref, rf_ref, xbuf, up_ref, e_ref, b_ref, k_ref, e_all, b_all, k_all,
          in_sem, e_send, e_recv, b_send, b_recv, k_send, k_recv):
    groups, tile, cols, width = x_hbm.shape
    steps = tile // SUBS
    n = SUBS * cols
    per = LANES // steps
    p, q = lax.axis_index("prow"), lax.axis_index("pcol")
    total = np_ * nq
    me = p * nq + q
    loads = [pltpu.make_async_copy(x_hbm.at[g], xbuf.at[g], in_sem.at[g]) for g in range(groups)]
    for load in loads:
        load.start()

    barrier = pltpu.get_barrier_semaphore()

    def greet(k, _):
        dev = lax.rem(me + k, total)
        pl.semaphore_signal(barrier, inc=1, device_id=(dev // nq, lax.rem(dev, nq)), device_id_type=MESH)
        return 0

    lax.fori_loop(1, total, greet, 0)

    u0, u1 = iotas(width, width)
    up_ref[...] = (u0 <= u1).astype(BF16)
    s0, lane = iotas(n, LANES)
    w0, _ = iotas(n, width)
    sub, _ = iotas(per * cols, width)

    def block(b, _):
        for k in range(per):
            g = b * per + k
            pltpu.make_async_copy(x_hbm.at[g], xbuf.at[g], in_sem.at[g]).wait()
        e = jnp.zeros((n, LANES), F32)
        bottom = jnp.zeros((per * cols, width), F32)
        for k in range(per):
            g = b * per + k
            x = xbuf[g].reshape(SUBS, steps, cols, width)
            x = jnp.swapaxes(x, 0, 1).reshape(steps * n, width)
            z = lax.dot_general(x, up_ref[...], NN, preferred_element_type=F32)
            acc = jnp.zeros((n, width), F32)
            for i in range(steps):
                acc = acc + z[i * n:(i + 1) * n]
                t_ref[g, pl.ds(i * n, n), :] = acc
                e = jnp.where(lane == k * steps + i, jnp.broadcast_to(acc[:, width - 1:], (n, LANES)), e)
            pt_ref[g] = shifted(acc, w0, cols, n)
            w = acc[:n // 2] + acc[n // 2:]
            w = w + pltpu.roll(w, cols, 0)
            w = w + pltpu.roll(w, 2 * cols, 0)
            bottom = jnp.where(sub // cols == k, w, bottom)
        down = shifted(e, s0, cols, n)
        for k in range(per):
            last = jnp.broadcast_to(down[:, (k + 1) * steps - 1:(k + 1) * steps], (n, LANES))
            e = e + jnp.where(lane // steps == k, last, 0.0)
        e_ref[b] = e
        b_ref[b] = bottom
        return 0

    lax.fori_loop(0, groups // per, block, 0)

    k0, k1 = iotas(per * cols, LANES)
    corner = jnp.zeros((per * cols, LANES), F32)
    for b in range(groups // per):
        edge = jnp.broadcast_to(b_ref[b][:, width - 1:], (per * cols, LANES))
        corner = jnp.where(k1 == b * per * cols + k0, edge, corner)
    k_ref[0] = jnp.sum(corner, axis=0, keepdims=True)
    pl.semaphore_wait(barrier, total - 1)

    def e_copy(k, sender, target):
        return pltpu.make_async_remote_copy(
            src_ref=e_ref, dst_ref=e_all.at[sender], send_sem=e_send.at[k], recv_sem=e_recv.at[sender],
            device_id=(p, target), device_id_type=MESH)

    def b_copy(k, sender, target):
        return pltpu.make_async_remote_copy(
            src_ref=b_ref, dst_ref=b_all.at[sender], send_sem=b_send.at[k], recv_sem=b_recv.at[sender],
            device_id=(target, q), device_id_type=MESH)

    def k_copy(k, sender, target):
        return pltpu.make_async_remote_copy(
            src_ref=k_ref.at[0], dst_ref=k_all.at[sender], send_sem=k_send.at[k], recv_sem=k_recv.at[sender],
            device_id=(target // nq, lax.rem(target, nq)), device_id_type=MESH)

    kinds = ((k_copy, me, total), (b_copy, p, np_), (e_copy, q, nq))
    for make, here, count in kinds:
        def send(k, _):
            make(k, here, lax.rem(here + k, count)).start()
            return 0
        lax.fori_loop(1, count, send, 0)

    def drain(make, here, count):
        def wait(k, _):
            make(k, lax.rem(here + k, count), lax.rem(here + k, count)).wait_recv()
            return 0
        lax.fori_loop(1, count, wait, 0)

    r0, _ = iotas(n, LANES)

    def factors(r, _):
        for i in range(steps):
            row = (r * np_ + p) * tile + (r0 // cols) * steps + i
            rf_ref[r, pl.ds(i * n, n), :] = 1.0 / jnp.sqrt((row + 1).astype(F32))
        return 0

    lax.fori_loop(0, rows_here, factors, 0)

    drain(*kinds[0])
    k_all[pl.ds(me, 1)] = k_ref[...]

    def k_sum(k, acc):
        a_all, a_lt, c_all, c_lt = acc
        value = k_all[k]
        kp, kq = k // nq, lax.rem(k, nq)
        left = jnp.where(kq < q, value, 0.0)
        up = jnp.where(kp < p, value, 0.0)
        both = jnp.where(kp < p, left, 0.0)
        return a_all + left, a_lt + both, c_all + value, c_lt + up

    zero = jnp.zeros((1, LANES), F32)
    a_all, a_lt, c_all, c_lt = lax.fori_loop(0, total, k_sum, (zero,) * 4)
    rows = groups * cols
    out, src = iotas(rows, LANES)
    out_g, src_g = out // cols, src // cols
    out_c, src_c = lax.rem(out, cols), lax.rem(src, cols)
    same_g = out_g == src_g
    above = (out_g // rows_here == src_g // rows_here) & (src_g < out_g)
    weigh = lambda strict, all_rows, lt_rows: (
        jnp.where(above & strict, all_rows, 0.0) + jnp.where(same_g & strict, lt_rows, 0.0))
    corner = jnp.sum(weigh(src_c == out_c, a_all, a_lt) + weigh(src_c < out_c, c_all, c_lt), axis=1, keepdims=True)

    drain(*kinds[1])
    s_all = b_ref[...].reshape(rows, width)
    s_lt = jnp.zeros_like(s_all)
    for k in range(np_):
        value = jnp.where(k == p, 0.0, b_all[k].reshape(rows, width))
        s_all = s_all + value
        s_lt = s_lt + jnp.where(k < p, value, 0.0)
    o, s = iotas(rows, rows)
    strict = ((o // (rows_here * cols) == s // (rows_here * cols)) & (lax.rem(o, cols) == lax.rem(s, cols))
              & (s // cols < o // cols)).astype(F32)
    pre = lax.dot_general(strict, s_all, NN, precision=HIGH, preferred_element_type=F32)
    d_ref[...] = (pre + s_lt + corner).reshape(groups // per, per * cols, width)

    drain(*kinds[2])
    flat = groups // per * n
    r_all = e_ref[...].reshape(flat, LANES)
    r_lt = jnp.zeros_like(r_all)
    for k in range(nq):
        value = jnp.where(k == q, 0.0, e_all[k].reshape(flat, LANES))
        r_all = r_all + value
        r_lt = r_lt + jnp.where(k < q, value, 0.0)
    f0, _ = iotas(flat, LANES)
    for shift in range(1, cols):
        r_lt = r_lt + jnp.where(lax.rem(f0, cols) >= shift, pltpu.roll(r_all, shift, 0), 0.0)
    c_ref[...] = r_lt.reshape(groups // per, n, LANES)

    for make, here, count in kinds:
        def sent(k, _):
            make(k, here, lax.rem(here + k, count)).wait_send()
            return 0
        lax.fori_loop(1, count, sent, 0)


def finish(np_, nq, rows_here, t_ref, pt_ref, c_ref, d_ref, rf_ref, out_hbm, obuf, cb_refs, sem):
    groups, rows, width = t_ref.shape
    cols = out_hbm.shape[3]
    n = SUBS * cols
    steps = rows // n
    per = LANES // steps
    lanes = width // LANES
    q = lax.axis_index("pcol")
    c0, c1 = iotas(n, width)
    cf = 1.0 / jnp.sqrt(((lax.rem(c0, cols) * nq + q) * width + c1 + 1).astype(F32))
    pitch = (steps + 1) * lanes
    sub, _ = iotas(per * cols, width)

    def copies(g):
        return [pltpu.make_async_copy(obuf.at[g, k, pl.ds(0, steps)], out_hbm.at[g, k // cols, :, k % cols], sem.at[g])
                for k in range(n)]

    def turned(g):
        return pltpu.roll(c_ref[g // per], LANES - lax.rem(g, per) * steps, 1)

    def spread(c, i):
        return jnp.broadcast_to(c[:, i:i + 1], (n, LANES))

    first = turned(0)
    for i in range(steps):
        cb_refs[0][pl.ds(i * n, n), :] = spread(first, i)

    def pair(b, ahead):
        for slot in range(2):
            g = b * 2 + slot
            r = lax.rem(g, rows_here)
            d = jnp.where(sub // cols == lax.rem(g, per), d_ref[g // per], 0.0)
            shift = cols
            while shift < per * cols:
                d = d + pltpu.roll(d, shift, 0)
                shift *= 2
            d = pt_ref[g] + jnp.concatenate([d] * (n // (per * cols)), axis=0)
            dst = obuf.at[g].reshape(n * pitch, LANES)
            later = turned(lax.rem(g + 2, groups))
            for i in range(steps):
                cb_refs[1 - slot][pl.ds(i * n, n), :] = spread(ahead, i)
            for i in range(steps):
                cut = pl.ds(i * n, n)
                cb, v, f = cb_refs[slot][cut, :], t_ref[g, cut, :], rf_ref[r, cut, :]
                for t in range(lanes):
                    col = slice(t * LANES, (t + 1) * LANES)
                    o = (v[:, col] + (cb + d[:, col])) * (f * cf[:, col])
                    for h in range(0, n, 8):
                        dst[pl.ds(h * pitch + i * lanes + t, 8, stride=pitch), :] = o[h:h + 8]
            ahead = later
            for copy in copies(g):
                copy.start()
        return ahead

    lax.fori_loop(0, groups // 2, pair, turned(1))

    def drain(g, _):
        pltpu.make_async_copy(out_hbm.at[g], out_hbm.at[g], sem.at[g]).wait()
        return 0

    lax.fori_loop(0, groups, drain, 0)


def solution(mesh):
    np_, nq = mesh.shape["prow"], mesh.shape["pcol"]

    def shards(matrix):
        batch, rows_here, _, tile, cols, _, width = matrix.shape
        groups, lanes = batch * rows_here, width // LANES
        steps, n, total = tile // SUBS, SUBS * cols, np_ * nq
        per = LANES // steps
        blocks = groups // per
        x = pltpu.with_memory_space_constraint(matrix.reshape(groups, tile, cols, width), pltpu.HBM)
        dma = pltpu.SemaphoreType.DMA
        vmem = pl.BlockSpec(memory_space=pltpu.VMEM)
        carried = pl.pallas_call(
            functools.partial(local, np_, nq, rows_here),
            out_shape=(jax.ShapeDtypeStruct((groups, tile * cols, width), F32),
                       jax.ShapeDtypeStruct((groups, n, width), F32),
                       jax.ShapeDtypeStruct((blocks, n, LANES), F32),
                       jax.ShapeDtypeStruct((blocks, per * cols, width), F32),
                       jax.ShapeDtypeStruct((rows_here, tile * cols, LANES), F32)),
            in_specs=[pl.BlockSpec(memory_space=pltpu.HBM)],
            out_specs=(vmem,) * 5,
            scratch_shapes=[
                pltpu.VMEM((groups, tile, cols, width), BF16),
                pltpu.VMEM((width, width), BF16),
                pltpu.VMEM((blocks, n, LANES), F32),
                pltpu.VMEM((blocks, per * cols, width), F32),
                pltpu.VMEM((1, 1, LANES), F32),
                pltpu.VMEM((nq, blocks, n, LANES), F32),
                pltpu.VMEM((np_, blocks, per * cols, width), F32),
                pltpu.VMEM((total, 1, LANES), F32),
                dma((groups,)), dma((nq,)), dma((nq,)), dma((np_,)), dma((np_,)), dma((total,)), dma((total,)),
            ],
            compiler_params=pltpu.CompilerParams(
                collective_id=0, has_side_effects=True, vmem_limit_bytes=24 * 2**20),
            name="local",
        )(x)
        out = pl.pallas_call(
            functools.partial(finish, np_, nq, rows_here),
            out_shape=jax.ShapeDtypeStruct((groups, SUBS, steps, cols, lanes, LANES), F32),
            in_specs=[vmem] * 5,
            out_specs=pl.BlockSpec(memory_space=pl.ANY),
            scratch_shapes=[
                pltpu.VMEM((groups, n, steps + 1, lanes, LANES), F32),
                [pltpu.VMEM((tile * cols, LANES), F32)] * 2,
                dma((groups,)),
            ],
            compiler_params=pltpu.CompilerParams(vmem_limit_bytes=24 * 2**20),
            name="finish",
        )(*carried)
        return out.reshape(matrix.shape)

    spec = P(None, None, "prow", None, None, "pcol", None)
    return jax.shard_map(shards, mesh=mesh, in_specs=(spec,), out_specs=spec, check_vma=False)
```

```python
import functools

import jax
import jax.numpy as jnp
from jax import lax
from jax.experimental import pallas as pl
from jax.experimental.pallas import tpu as pltpu
from jax.sharding import PartitionSpec as P

F32, BF16 = jnp.float32, jnp.bfloat16
HIGH = lax.Precision.HIGHEST
MESH = pl.DeviceIdType.MESH
NN = (((1,), (0,)), ((), ()))
SUBS = 8
LANES = 128
CHUNKS = 2


def iotas(rows, cols):
    return (lax.broadcasted_iota(jnp.int32, (rows, cols), 0), lax.broadcasted_iota(jnp.int32, (rows, cols), 1))


def shifted(v, rows, cols, count):
    v = jnp.where(rows >= cols, pltpu.roll(v, cols, 0), 0.0)
    shift = cols
    while shift < count:
        v = v + jnp.where(rows >= shift, pltpu.roll(v, shift, 0), 0.0)
        shift *= 2
    return v


def local(np_, nq, rows_here, x_hbm, t_ref, pt_ref, c_ref, d_ref, rf_ref, xbuf, up_ref, e_tmp, e_ref, b_ref, k_ref,
          e_all, b_all, k_all, in_sem, e_send, e_recv, f_send, f_recv, b_send, b_recv, k_send, k_recv):
    groups, tile, cols, width = x_hbm.shape
    steps = tile // SUBS
    n = SUBS * cols
    per = LANES // steps
    blocks = groups // per
    chunks, _, part = e_ref.shape[:3]
    p, q = lax.axis_index("prow"), lax.axis_index("pcol")
    total = np_ * nq
    me = p * nq + q
    loads = [pltpu.make_async_copy(x_hbm.at[g], xbuf.at[g], in_sem.at[g]) for g in range(groups)]
    for load in loads:
        load.start()

    def around(i, j):
        return lax.rem(p + i, np_), lax.rem(q + j, nq)

    def others(visit):
        for j in range(1, nq):
            visit(p, lax.rem(q + j, nq), j)

        def row(i, _):
            for j in range(nq):
                visit(*around(i, j), i * nq + j)
            return 0

        lax.fori_loop(1, np_, row, 0)

    barrier = pltpu.get_barrier_semaphore()
    others(lambda tp, tq, k: pl.semaphore_signal(barrier, inc=1, device_id=(tp, tq), device_id_type=MESH))

    u0, u1 = iotas(width, width)
    up_ref[...] = (u0 <= u1).astype(BF16)
    s0, lane = iotas(n, LANES)
    w0, _ = iotas(n, width)
    sub, _ = iotas(per * cols, width)

    def block(b, h):
        for k in range(per):
            g = b * per + k
            pltpu.make_async_copy(x_hbm.at[g], xbuf.at[g], in_sem.at[g]).wait()
        e = jnp.zeros((n, LANES), F32)
        bottom = jnp.zeros((per * cols, width), F32)
        for k in range(per):
            g = b * per + k
            x = xbuf[g].reshape(SUBS, steps, cols, width)
            x = jnp.swapaxes(x, 0, 1).reshape(steps * n, width)
            z = lax.dot_general(x, up_ref[...], NN, preferred_element_type=F32)
            acc = jnp.zeros((n, width), F32)
            for i in range(steps):
                acc = acc + z[i * n:(i + 1) * n]
                t_ref[g, pl.ds(i * n, n), :] = acc
                e = jnp.where(lane == k * steps + i, jnp.broadcast_to(acc[:, width - 1:], (n, LANES)), e)
            pt_ref[g] = shifted(acc, w0, cols, n)
            w = acc[:n // 2] + acc[n // 2:]
            w = w + pltpu.roll(w, cols, 0)
            w = w + pltpu.roll(w, 2 * cols, 0)
            bottom = jnp.where(sub // cols == k, w, bottom)
        down = shifted(e, s0, cols, n)
        for k in range(per):
            last = jnp.broadcast_to(down[:, (k + 1) * steps - 1:(k + 1) * steps], (n, LANES))
            e = e + jnp.where(lane // steps == k, last, 0.0)
        e_tmp[...] = e
        for c in range(cols):
            e_ref[h, c, b - h * part] = e_tmp[pl.ds(c, SUBS, stride=cols), :]
        b_ref[b] = bottom
        return h

    def most(h, k, sender, target):
        return pltpu.make_async_remote_copy(
            src_ref=e_ref.at[h, pl.ds(0, cols - 1)], dst_ref=e_all.at[sender, h, pl.ds(0, cols - 1)],
            send_sem=e_send.at[h, k], recv_sem=e_recv.at[h, sender], device_id=(p, target), device_id_type=MESH)

    def last(h, k, sender, target):
        return pltpu.make_async_remote_copy(
            src_ref=e_ref.at[h, cols - 1], dst_ref=e_all.at[sender, h, cols - 1],
            send_sem=f_send.at[h, k], recv_sem=f_recv.at[h, sender], device_id=(p, target), device_id_type=MESH)

    def b_copy(k, sender, target):
        return pltpu.make_async_remote_copy(
            src_ref=b_ref, dst_ref=b_all.at[sender], send_sem=b_send.at[k], recv_sem=b_recv.at[sender],
            device_id=(target, q), device_id_type=MESH)

    def k_copy(tp, tq, k):
        return pltpu.make_async_remote_copy(
            src_ref=k_ref.at[0], dst_ref=k_all.at[me], send_sem=k_send.at[k], recv_sem=k_recv,
            device_id=(tp, tq), device_id_type=MESH)

    def send_edges(h):
        for k in range(1, nq):
            target = lax.rem(q + k, nq)
            most(h, k, q, target).start()

            @pl.when(target > q)
            def _():
                last(h, k, q, target).start()

    late = 4 * q >= 3 * nq

    def meet():
        pl.semaphore_wait(barrier, total - 1)
        for h in range(chunks - 1):
            send_edges(h)

    for h in range(chunks):
        if h == chunks - 1:
            pl.when(late)(meet)
        lax.fori_loop(h * part, (h + 1) * part, block, h)
    pl.when(jnp.logical_not(late))(meet)

    k0, k1 = iotas(per * cols, LANES)
    corner = jnp.zeros((per * cols, LANES), F32)
    for b in range(blocks):
        edge = jnp.broadcast_to(b_ref[b][:, width - 1:], (per * cols, LANES))
        corner = jnp.where(k1 == b * per * cols + k0, edge, corner)
    k_ref[0] = jnp.sum(corner, axis=0, keepdims=True)
    k_all[pl.ds(me, 1)] = k_ref[...]
    others(lambda tp, tq, k: k_copy(tp, tq, k).start())
    send_edges(chunks - 1)
    for k in range(1, np_):
        b_copy(k, p, lax.rem(p + k, np_)).start()

    r0, _ = iotas(n, LANES)

    def factors(r, _):
        for i in range(steps):
            row = (r * np_ + p) * tile + (r0 // cols) * steps + i
            rf_ref[r, pl.ds(i * n, n), :] = 1.0 / jnp.sqrt((row + 1).astype(F32))
        return 0

    lax.fori_loop(0, rows_here, factors, 0)

    for k in range(1, np_):
        sender = lax.rem(p + k, np_)
        b_copy(k, sender, sender).wait_recv()
    rows = groups * cols
    s_all = b_ref[...].reshape(rows, width)
    s_lt = jnp.zeros_like(s_all)
    for k in range(np_):
        value = jnp.where(k == p, 0.0, b_all[k].reshape(rows, width))
        s_all = s_all + value
        s_lt = s_lt + jnp.where(k < p, value, 0.0)
    o, s = iotas(rows, rows)
    strict = ((o // (rows_here * cols) == s // (rows_here * cols)) & (lax.rem(o, cols) == lax.rem(s, cols))
              & (s // cols < o // cols)).astype(F32)
    pre = lax.dot_general(strict, s_all, NN, precision=HIGH, preferred_element_type=F32)
    d_ref[...] = (pre + s_lt).reshape(blocks, per * cols, width)

    for h in range(chunks):
        for k in range(1, nq):
            sender = lax.rem(q + k, nq)
            most(h, k, sender, sender).wait_recv()

            @pl.when(sender < q)
            def _():
                last(h, k, sender, sender).wait_recv()

        base = jnp.zeros((part, SUBS, LANES), F32)
        for c in range(cols):
            whole, before = e_ref[h, c], jnp.zeros((part, SUBS, LANES), F32)
            for k in range(nq):
                value = e_all[k, h, c]
                before = before + jnp.where(k < q, value, 0.0)
                if c < cols - 1:
                    whole = whole + jnp.where(k == q, 0.0, value)
            for b in range(part):
                c_ref[h * part + b, pl.ds(c, SUBS, stride=cols), :] = (base + before)[b]
            base = base + whole

    others(lambda tp, tq, k: k_copy(tp, tq, k).wait_send())
    for k in range(1, np_):
        b_copy(k, p, p).wait_send()
    for h in range(chunks):
        for k in range(1, nq):
            target = lax.rem(q + k, nq)
            most(h, k, q, target).wait_send()

            @pl.when(target > q)
            def _():
                last(h, k, q, target).wait_send()

    pltpu.make_async_copy(k_all.at[pl.ds(0, total - 1)], k_all.at[pl.ds(0, total - 1)], k_recv).wait()
    value = k_all.reshape(total, LANES)[...]
    d0, _ = iotas(total, LANES)
    left = jnp.where(lax.rem(d0, nq) < q, value, 0.0)
    add = lambda v: jnp.sum(v, axis=0, keepdims=True)
    a_all, a_lt = add(left), add(jnp.where(d0 // nq < p, left, 0.0))
    c_all, c_lt = add(value), add(jnp.where(d0 // nq < p, value, 0.0))
    out, src = iotas(rows, LANES)
    out_g, src_g = out // cols, src // cols
    out_c, src_c = lax.rem(out, cols), lax.rem(src, cols)
    same_g = out_g == src_g
    above = (out_g // rows_here == src_g // rows_here) & (src_g < out_g)
    weigh = lambda strict, all_rows, lt_rows: (
        jnp.where(above & strict, all_rows, 0.0) + jnp.where(same_g & strict, lt_rows, 0.0))
    corner = jnp.sum(weigh(src_c == out_c, a_all, a_lt) + weigh(src_c < out_c, c_all, c_lt), axis=1, keepdims=True)
    d_ref[...] = d_ref[...] + corner.reshape(blocks, per * cols, 1)


def finish(np_, nq, rows_here, t_ref, pt_ref, c_ref, d_ref, rf_ref, out_hbm, obuf, cb_refs, sem):
    groups, rows, width = t_ref.shape
    cols = out_hbm.shape[3]
    n = SUBS * cols
    steps = rows // n
    per = LANES // steps
    lanes = width // LANES
    q = lax.axis_index("pcol")
    c0, c1 = iotas(n, width)
    cf = 1.0 / jnp.sqrt(((lax.rem(c0, cols) * nq + q) * width + c1 + 1).astype(F32))
    pitch = (steps + 1) * lanes
    sub, _ = iotas(per * cols, width)

    def copies(g):
        return [pltpu.make_async_copy(obuf.at[g, k, pl.ds(0, steps)], out_hbm.at[g, k // cols, :, k % cols], sem.at[g])
                for k in range(n)]

    def turned(g):
        return pltpu.roll(c_ref[g // per], LANES - lax.rem(g, per) * steps, 1)

    def spread(c, i):
        return jnp.broadcast_to(c[:, i:i + 1], (n, LANES))

    first = turned(0)
    for i in range(steps):
        cb_refs[0][pl.ds(i * n, n), :] = spread(first, i)

    def pair(b, ahead):
        for slot in range(2):
            g = b * 2 + slot
            r = lax.rem(g, rows_here)
            d = jnp.where(sub // cols == lax.rem(g, per), d_ref[g // per], 0.0)
            shift = cols
            while shift < per * cols:
                d = d + pltpu.roll(d, shift, 0)
                shift *= 2
            d = pt_ref[g] + jnp.concatenate([d] * (n // (per * cols)), axis=0)
            dst = obuf.at[g].reshape(n * pitch, LANES)
            later = turned(lax.rem(g + 2, groups))
            for i in range(steps):
                cb_refs[1 - slot][pl.ds(i * n, n), :] = spread(ahead, i)
            for i in range(steps):
                cut = pl.ds(i * n, n)
                cb, v, f = cb_refs[slot][cut, :], t_ref[g, cut, :], rf_ref[r, cut, :]
                for t in range(lanes):
                    col = slice(t * LANES, (t + 1) * LANES)
                    o = (v[:, col] + (cb + d[:, col])) * (f * cf[:, col])
                    for h in range(0, n, 8):
                        dst[pl.ds(h * pitch + i * lanes + t, 8, stride=pitch), :] = o[h:h + 8]
            ahead = later
            for copy in copies(g):
                copy.start()
        return ahead

    lax.fori_loop(0, groups // 2, pair, turned(1))

    def drain(g, _):
        pltpu.make_async_copy(out_hbm.at[g], out_hbm.at[g], sem.at[g]).wait()
        return 0

    lax.fori_loop(0, groups, drain, 0)


def solution(mesh):
    np_, nq = mesh.shape["prow"], mesh.shape["pcol"]

    def shards(matrix):
        batch, rows_here, _, tile, cols, _, width = matrix.shape
        groups, lanes = batch * rows_here, width // LANES
        steps, n, total = tile // SUBS, SUBS * cols, np_ * nq
        per = LANES // steps
        blocks = groups // per
        x = pltpu.with_memory_space_constraint(matrix.reshape(groups, tile, cols, width), pltpu.HBM)
        dma = pltpu.SemaphoreType.DMA
        vmem = pl.BlockSpec(memory_space=pltpu.VMEM)
        carried = pl.pallas_call(
            functools.partial(local, np_, nq, rows_here),
            out_shape=(jax.ShapeDtypeStruct((groups, tile * cols, width), F32),
                       jax.ShapeDtypeStruct((groups, n, width), F32),
                       jax.ShapeDtypeStruct((blocks, n, LANES), F32),
                       jax.ShapeDtypeStruct((blocks, per * cols, width), F32),
                       jax.ShapeDtypeStruct((rows_here, tile * cols, LANES), F32)),
            in_specs=[pl.BlockSpec(memory_space=pltpu.HBM)],
            out_specs=(vmem,) * 5,
            scratch_shapes=[
                pltpu.VMEM((groups, tile, cols, width), BF16),
                pltpu.VMEM((width, width), BF16),
                pltpu.VMEM((n, LANES), F32),
                pltpu.VMEM((CHUNKS, cols, blocks // CHUNKS, SUBS, LANES), F32),
                pltpu.VMEM((blocks, per * cols, width), F32),
                pltpu.VMEM((1, 1, LANES), F32),
                pltpu.VMEM((nq, CHUNKS, cols, blocks // CHUNKS, SUBS, LANES), F32),
                pltpu.VMEM((np_, blocks, per * cols, width), F32),
                pltpu.VMEM((total, 1, LANES), F32),
                dma((groups,)), dma((CHUNKS, nq)), dma((CHUNKS, nq)), dma((CHUNKS, nq)), dma((CHUNKS, nq)),
                dma((np_,)), dma((np_,)), dma((total,)), dma,
            ],
            compiler_params=pltpu.CompilerParams(
                collective_id=0, has_side_effects=True, vmem_limit_bytes=24 * 2**20),
            name="local",
        )(x)
        out = pl.pallas_call(
            functools.partial(finish, np_, nq, rows_here),
            out_shape=jax.ShapeDtypeStruct((groups, SUBS, steps, cols, lanes, LANES), F32),
            in_specs=[vmem] * 5,
            out_specs=pl.BlockSpec(memory_space=pl.ANY),
            scratch_shapes=[
                pltpu.VMEM((groups, n, steps + 1, lanes, LANES), F32),
                [pltpu.VMEM((tile * cols, LANES), F32)] * 2,
                dma((groups,)),
            ],
            compiler_params=pltpu.CompilerParams(vmem_limit_bytes=24 * 2**20),
            name="finish",
        )(*carried)
        return out.reshape(matrix.shape)

    spec = P(None, None, "prow", None, None, "pcol", None)
    return jax.shard_map(shards, mesh=mesh, in_specs=(spec,), out_specs=spec, check_vma=False)
```

```python
import functools

import jax
import jax.numpy as jnp
from jax import lax
from jax.experimental import pallas as pl
from jax.experimental.pallas import tpu as pltpu
from jax.sharding import PartitionSpec as P

F32, BF16 = jnp.float32, jnp.bfloat16
HIGH = lax.Precision.HIGHEST
MESH = pl.DeviceIdType.MESH
NN = (((1,), (0,)), ((), ()))
SUBS = 8
LANES = 128


def iotas(rows, cols):
    return (lax.broadcasted_iota(jnp.int32, (rows, cols), 0), lax.broadcasted_iota(jnp.int32, (rows, cols), 1))


def shifted(v, rows, cols, count):
    v = jnp.where(rows >= cols, pltpu.roll(v, cols, 0), 0.0)
    shift = cols
    while shift < count:
        v = v + jnp.where(rows >= shift, pltpu.roll(v, shift, 0), 0.0)
        shift *= 2
    return v


def local(np_, nq, rows_here, x_hbm, t_ref, pt_ref, c_ref, d_ref, rf_ref, xbuf, up_ref, e_tmp, e_ref, b_ref, k_ref,
          e_all, b_all, k_all, in_sem, e_send, e_recv, b_send, b_recv, k_send, k_recv):
    groups, tile, cols, width = x_hbm.shape
    steps = tile // SUBS
    n = SUBS * cols
    per = LANES // steps
    blocks = groups // per
    p, q = lax.axis_index("prow"), lax.axis_index("pcol")
    total = np_ * nq
    me = p * nq + q
    for g in range(groups):
        pltpu.make_async_copy(x_hbm.at[g], xbuf.at[g], in_sem.at[g // per]).start()

    def around(i, j):
        return lax.rem(p + i, np_), lax.rem(q + j, nq)

    def others(visit):
        for j in range(1, nq):
            visit(p, lax.rem(q + j, nq), j)

        def row(i, _):
            for j in range(nq):
                visit(*around(i, j), i * nq + j)
            return 0

        lax.fori_loop(1, np_, row, 0)

    barrier = pltpu.get_barrier_semaphore()
    others(lambda tp, tq, k: pl.semaphore_signal(barrier, inc=1, device_id=(tp, tq), device_id_type=MESH))

    u0, u1 = iotas(width, width)
    up_ref[...] = (u0 <= u1).astype(BF16)
    s0, lane = iotas(n, LANES)
    w0, _ = iotas(n, width)
    sub, _ = iotas(per * cols, width)

    def arrive(b):
        part = pl.ds(b * per, per)
        pltpu.make_async_copy(x_hbm.at[part], xbuf.at[part], in_sem.at[b]).wait()

    def block(b):
        bottom = jnp.zeros((per * cols, width), F32)
        for k in range(per):
            g = b * per + k
            x = xbuf[g].reshape(SUBS, steps, cols, width)
            x = jnp.swapaxes(x, 0, 1).reshape(steps * n, width)
            z = lax.dot_general(x, up_ref[...], NN, preferred_element_type=F32)
            acc = jnp.zeros((n, width), F32)
            for i in range(steps):
                acc = acc + z[i * n:(i + 1) * n]
                t_ref[g, pl.ds(i * n, n), :] = acc
            pt_ref[g] = shifted(acc, w0, cols, n)
            w = acc[:n // 2] + acc[n // 2:]
            w = w + pltpu.roll(w, cols, 0)
            w = w + pltpu.roll(w, 2 * cols, 0)
            bottom = jnp.where(sub // cols == k, w, bottom)
        b_ref[b] = bottom

    def side_of(b):
        e = jnp.zeros((n, LANES), F32)
        for k in range(per):
            for i in range(steps):
                side = t_ref[b * per + k, pl.ds(i * n, n), pl.ds(width - LANES, LANES)]
                e = jnp.where(lane == k * steps + i, jnp.broadcast_to(side[:, LANES - 1:], (n, LANES)), e)
        down = shifted(e, s0, cols, n)
        for k in range(per):
            last = jnp.broadcast_to(down[:, (k + 1) * steps - 1:(k + 1) * steps], (n, LANES))
            e = e + jnp.where(lane // steps == k, last, 0.0)
        e_tmp[...] = e
        for c in range(cols):
            e_ref[b, c] = e_tmp[pl.ds(c, SUBS, stride=cols), :]

    def up(part, sender, target):
        return pltpu.make_async_remote_copy(
            src_ref=e_ref.at[part], dst_ref=e_all.at[sender, part], send_sem=e_send.at[target],
            recv_sem=e_recv.at[(part.start + part.size) // blocks, sender], device_id=(p, target), device_id_type=MESH)

    def down(part, sender, target):
        return pltpu.make_async_remote_copy(
            src_ref=e_ref.at[part, pl.ds(0, cols - 1)], dst_ref=e_all.at[sender, part, pl.ds(0, cols - 1)],
            send_sem=e_send.at[target], recv_sem=e_recv.at[(part.start + part.size) // blocks, sender],
            device_id=(p, target), device_id_type=MESH)

    def when(cond, act):
        @pl.when(cond)
        def _():
            act()

    def b_copy(k, sender, target):
        return pltpu.make_async_remote_copy(
            src_ref=b_ref, dst_ref=b_all.at[sender], send_sem=b_send, recv_sem=b_recv,
            device_id=(target, q), device_id_type=MESH)

    def k_copy(tp, tq, k):
        return pltpu.make_async_remote_copy(
            src_ref=k_ref.at[0], dst_ref=k_all.at[me], send_sem=k_send, recv_sem=k_recv,
            device_id=(tp, tq), device_id_type=MESH)

    def send_edges(begin, end):
        part = pl.ds(begin, end - begin)
        for k in range(nq):
            far = nq - 1 - k
            when(far > q, lambda: up(part, q, far).start())
            when(k < q, lambda: down(part, q, k).start())

    late = 4 * q >= 3 * nq

    def meet(begin, end):
        pl.semaphore_wait(barrier, total - 1)
        send_edges(begin, end)

    arrive(0)
    block(0)
    for b in range(1, blocks):
        arrive(b)
        block(b)
        side_of(b - 1)
        if b == blocks - 2:
            when(late, lambda: meet(0, b))
    when(jnp.logical_not(late), lambda: meet(0, blocks - 2))

    k0, k1 = iotas(per * cols, LANES)
    corner = jnp.zeros((per * cols, LANES), F32)
    for b in range(blocks):
        edge = jnp.broadcast_to(b_ref[b][:, width - 1:], (per * cols, LANES))
        corner = jnp.where(k1 == b * per * cols + k0, edge, corner)
    k_ref[0] = jnp.sum(corner, axis=0, keepdims=True)
    k_all[pl.ds(me, 1)] = k_ref[...]
    others(lambda tp, tq, k: k_copy(tp, tq, k).start())
    send_edges(blocks - 2, blocks - 1)
    side_of(blocks - 1)
    send_edges(blocks - 1, blocks)
    for k in range(1, np_):
        b_copy(k, p, lax.rem(p + k, np_)).start()

    r0, _ = iotas(n, LANES)

    def factors(r, _):
        for i in range(steps):
            row = (r * np_ + p) * tile + (r0 // cols) * steps + i
            rf_ref[r, pl.ds(i * n, n), :] = 1.0 / jnp.sqrt((row + 1).astype(F32))
        return 0

    lax.fori_loop(0, rows_here, factors, 0)

    pltpu.make_async_copy(b_all.at[pl.ds(0, np_ - 1)], b_all.at[pl.ds(0, np_ - 1)], b_recv).wait()
    rows = groups * cols
    s_all = b_ref[...].reshape(rows, width)
    s_lt = jnp.zeros_like(s_all)
    for k in range(np_):
        value = jnp.where(k == p, 0.0, b_all[k].reshape(rows, width))
        s_all = s_all + value
        s_lt = s_lt + jnp.where(k < p, value, 0.0)
    o, s = iotas(rows, rows)
    strict = ((o // (rows_here * cols) == s // (rows_here * cols)) & (lax.rem(o, cols) == lax.rem(s, cols))
              & (s // cols < o // cols)).astype(F32)
    pre = lax.dot_general(strict, s_all, NN, precision=HIGH, preferred_element_type=F32)
    d_ref[...] = (pre + s_lt).reshape(blocks, per * cols, width)

    def sums(b):
        base = jnp.zeros((SUBS, LANES), F32)
        for c in range(cols):
            whole, before = e_ref[b, c], jnp.zeros((SUBS, LANES), F32)
            for k in range(nq):
                value = e_all[k, b, c]
                before = before + jnp.where(k < q, value, 0.0)
                if c < cols - 1:
                    whole = whole + jnp.where(k == q, 0.0, value)
            c_ref[b, pl.ds(c, SUBS, stride=cols), :] = base + before
            base = base + whole

    def collect(begin, end):
        part = pl.ds(begin, end - begin)
        for k in range(nq):
            when(k < q, lambda: up(part, k, k).wait_recv())
            when(k > q, lambda: down(part, k, k).wait_recv())
        for b in range(begin, end):
            sums(b)

    collect(0, blocks - 1)
    pltpu.make_async_copy(k_all.at[pl.ds(0, total - 1)], k_all.at[pl.ds(0, total - 1)], k_send).wait()
    pltpu.make_async_copy(b_all.at[pl.ds(0, np_ - 1)], b_all.at[pl.ds(0, np_ - 1)], b_send).wait()
    for k in range(nq):
        when(k > q, lambda: up(pl.ds(0, blocks), q, k).wait_send())
        when(k < q, lambda: down(pl.ds(0, blocks), q, k).wait_send())
    collect(blocks - 1, blocks)

    pltpu.make_async_copy(k_all.at[pl.ds(0, total - 1)], k_all.at[pl.ds(0, total - 1)], k_recv).wait()
    value = k_all.reshape(total, LANES)[...]
    d0, _ = iotas(total, LANES)
    left = jnp.where(lax.rem(d0, nq) < q, value, 0.0)
    add = lambda v: jnp.sum(v, axis=0, keepdims=True)
    a_all, a_lt = add(left), add(jnp.where(d0 // nq < p, left, 0.0))
    c_all, c_lt = add(value), add(jnp.where(d0 // nq < p, value, 0.0))
    out, src = iotas(rows, LANES)
    out_g, src_g = out // cols, src // cols
    out_c, src_c = lax.rem(out, cols), lax.rem(src, cols)
    same_g = out_g == src_g
    above = (out_g // rows_here == src_g // rows_here) & (src_g < out_g)
    weigh = lambda strict, all_rows, lt_rows: (
        jnp.where(above & strict, all_rows, 0.0) + jnp.where(same_g & strict, lt_rows, 0.0))
    corner = jnp.sum(weigh(src_c == out_c, a_all, a_lt) + weigh(src_c < out_c, c_all, c_lt), axis=1, keepdims=True)
    d_ref[...] = d_ref[...] + corner.reshape(blocks, per * cols, 1)


def finish(np_, nq, rows_here, t_ref, pt_ref, c_ref, d_ref, rf_ref, out_hbm, obuf, cb_refs, sem):
    groups, rows, width = t_ref.shape
    cols = out_hbm.shape[3]
    n = SUBS * cols
    steps = rows // n
    per = LANES // steps
    lanes = width // LANES
    q = lax.axis_index("pcol")
    c0, c1 = iotas(n, width)
    cf = 1.0 / jnp.sqrt(((lax.rem(c0, cols) * nq + q) * width + c1 + 1).astype(F32))
    pitch = (steps + 1) * lanes
    sub, _ = iotas(per * cols, width)

    def copies(g):
        return [pltpu.make_async_copy(obuf.at[g, k, pl.ds(0, steps)], out_hbm.at[g, k // cols, :, k % cols], sem)
                for k in range(n)]

    def turned(g):
        return pltpu.roll(c_ref[g // per], LANES - lax.rem(g, per) * steps, 1)

    def spread(c, i):
        return jnp.broadcast_to(c[:, i:i + 1], (n, LANES))

    first = turned(0)
    for i in range(steps):
        cb_refs[0][pl.ds(i * n, n), :] = spread(first, i)

    def pair(b, ahead):
        for slot in range(2):
            g = b * 2 + slot
            r = lax.rem(g, rows_here)
            d = jnp.where(sub // cols == lax.rem(g, per), d_ref[g // per], 0.0)
            shift = cols
            while shift < per * cols:
                d = d + pltpu.roll(d, shift, 0)
                shift *= 2
            d = pt_ref[g] + jnp.concatenate([d] * (n // (per * cols)), axis=0)
            dst = obuf.at[g].reshape(n * pitch, LANES)
            later = turned(lax.rem(g + 2, groups))
            for i in range(steps):
                cb_refs[1 - slot][pl.ds(i * n, n), :] = spread(ahead, i)
            for i in range(steps):
                cut = pl.ds(i * n, n)
                cb, v, f = cb_refs[slot][cut, :], t_ref[g, cut, :], rf_ref[r, cut, :]
                for t in range(lanes):
                    col = slice(t * LANES, (t + 1) * LANES)
                    o = (v[:, col] + (cb + d[:, col])) * (f * cf[:, col])
                    for h in range(0, n, 8):
                        dst[pl.ds(h * pitch + i * lanes + t, 8, stride=pitch), :] = o[h:h + 8]
            ahead = later
            for copy in copies(g):
                copy.start()
        return ahead

    lax.fori_loop(0, groups // 2, pair, turned(1))

    pltpu.make_async_copy(out_hbm, out_hbm, sem).wait()


def solution(mesh):
    np_, nq = mesh.shape["prow"], mesh.shape["pcol"]

    def shards(matrix):
        batch, rows_here, _, tile, cols, _, width = matrix.shape
        groups, lanes = batch * rows_here, width // LANES
        steps, n, total = tile // SUBS, SUBS * cols, np_ * nq
        per = LANES // steps
        blocks = groups // per
        x = pltpu.with_memory_space_constraint(matrix.reshape(groups, tile, cols, width), pltpu.HBM)
        dma = pltpu.SemaphoreType.DMA
        vmem = pl.BlockSpec(memory_space=pltpu.VMEM)
        carried = pl.pallas_call(
            functools.partial(local, np_, nq, rows_here),
            out_shape=(jax.ShapeDtypeStruct((groups, tile * cols, width), F32),
                       jax.ShapeDtypeStruct((groups, n, width), F32),
                       jax.ShapeDtypeStruct((blocks, n, LANES), F32),
                       jax.ShapeDtypeStruct((blocks, per * cols, width), F32),
                       jax.ShapeDtypeStruct((rows_here, tile * cols, LANES), F32)),
            in_specs=[pl.BlockSpec(memory_space=pltpu.HBM)],
            out_specs=(vmem,) * 5,
            scratch_shapes=[
                pltpu.VMEM((groups, tile, cols, width), BF16),
                pltpu.VMEM((width, width), BF16),
                pltpu.VMEM((n, LANES), F32),
                pltpu.VMEM((blocks, cols, SUBS, LANES), F32),
                pltpu.VMEM((blocks, per * cols, width), F32),
                pltpu.VMEM((1, 1, LANES), F32),
                pltpu.VMEM((nq, blocks, cols, SUBS, LANES), F32),
                pltpu.VMEM((np_, blocks, per * cols, width), F32),
                pltpu.VMEM((total, 1, LANES), F32),
                dma((blocks,)), dma((nq,)), dma((2, nq)), dma, dma, dma, dma,
            ],
            compiler_params=pltpu.CompilerParams(
                collective_id=0, has_side_effects=True, vmem_limit_bytes=24 * 2**20),
            name="local",
        )(x)
        out = pl.pallas_call(
            functools.partial(finish, np_, nq, rows_here),
            out_shape=jax.ShapeDtypeStruct((groups, SUBS, steps, cols, lanes, LANES), F32),
            in_specs=[vmem] * 5,
            out_specs=pl.BlockSpec(memory_space=pl.ANY),
            scratch_shapes=[
                pltpu.VMEM((groups, n, steps + 1, lanes, LANES), F32),
                [pltpu.VMEM((tile * cols, LANES), F32)] * 2,
                dma,
            ],
            compiler_params=pltpu.CompilerParams(vmem_limit_bytes=24 * 2**20),
            name="finish",
        )(*carried)
        return out.reshape(matrix.shape)

    spec = P(None, None, "prow", None, None, "pcol", None)
    return jax.shard_map(shards, mesh=mesh, in_specs=(spec,), out_specs=spec, check_vma=False)
```

```python
import functools

import jax
import jax.numpy as jnp
from jax import lax
from jax.experimental import pallas as pl
from jax.experimental.pallas import tpu as pltpu
from jax.sharding import PartitionSpec as P

F32, BF16 = jnp.float32, jnp.bfloat16
HIGH = lax.Precision.HIGHEST
MESH = pl.DeviceIdType.MESH
NN = (((1,), (0,)), ((), ()))
SUBS = 8
LANES = 128


def iotas(rows, cols):
    return (lax.broadcasted_iota(jnp.int32, (rows, cols), 0), lax.broadcasted_iota(jnp.int32, (rows, cols), 1))


def shifted(v, rows, cols, count):
    v = jnp.where(rows >= cols, pltpu.roll(v, cols, 0), 0.0)
    shift = cols
    while shift < count:
        v = v + jnp.where(rows >= shift, pltpu.roll(v, shift, 0), 0.0)
        shift *= 2
    return v


def local(np_, nq, rows_here, x_hbm, t_ref, pt_ref, c_ref, d_ref, rf_ref, xbuf, up_ref, e_tmp, e_ref, b_ref, k_ref,
          e_all, b_all, k_all, in_sem, e_send, e_recv, b_send, b_recv, k_send, k_recv):
    groups, tile, cols, width = x_hbm.shape
    steps = tile // SUBS
    n = SUBS * cols
    per = LANES // steps
    blocks = groups // per
    p, q = lax.axis_index("prow"), lax.axis_index("pcol")
    total = np_ * nq
    me = p * nq + q
    for g in range(groups):
        pltpu.make_async_copy(x_hbm.at[g], xbuf.at[g], in_sem.at[g // per]).start()

    def others(visit):
        def column(k, _):
            target = jnp.where(k < q, k, nq - 1 - (k - q))
            for i in range(np_):
                visit(lax.rem(p + i, np_), target)
            return 0

        lax.fori_loop(0, nq - 1, column, 0)
        for i in range(1, np_):
            visit(lax.rem(p + i, np_), q)

    barrier = pltpu.get_barrier_semaphore()
    others(lambda tp, tq: pl.semaphore_signal(barrier, inc=1, device_id=(tp, tq), device_id_type=MESH))

    u0, u1 = iotas(width, width)
    up_ref[...] = (u0 <= u1).astype(BF16)
    s0, lane = iotas(n, LANES)
    w0, _ = iotas(n, width)
    sub, _ = iotas(per * cols, width)

    def arrive(b):
        part = pl.ds(b * per, per)
        pltpu.make_async_copy(x_hbm.at[part], xbuf.at[part], in_sem.at[b]).wait()

    def block(b):
        bottom = jnp.zeros((per * cols, width), F32)
        for k in range(per):
            g = b * per + k
            x = xbuf[g].reshape(SUBS, steps, cols, width)
            x = jnp.swapaxes(x, 0, 1).reshape(steps * n, width)
            z = lax.dot_general(x, up_ref[...], NN, preferred_element_type=F32)
            acc = jnp.zeros((n, width), F32)
            for i in range(steps):
                acc = acc + z[i * n:(i + 1) * n]
                t_ref[g, pl.ds(i * n, n), :] = acc
            pt_ref[g] = shifted(acc, w0, cols, n)
            w = acc[:n // 2] + acc[n // 2:]
            w = w + pltpu.roll(w, cols, 0)
            w = w + pltpu.roll(w, 2 * cols, 0)
            bottom = jnp.where(sub // cols == k, w, bottom)
        b_ref[b] = bottom

    def side_of(b):
        e = jnp.zeros((n, LANES), F32)
        for k in range(per):
            for i in range(steps):
                side = t_ref[b * per + k, pl.ds(i * n, n), pl.ds(width - LANES, LANES)]
                e = jnp.where(lane == k * steps + i, jnp.broadcast_to(side[:, LANES - 1:], (n, LANES)), e)
        down = shifted(e, s0, cols, n)
        for k in range(per):
            last = jnp.broadcast_to(down[:, (k + 1) * steps - 1:(k + 1) * steps], (n, LANES))
            e = e + jnp.where(lane // steps == k, last, 0.0)
        e_tmp[...] = e
        for c in range(cols):
            e_ref[b, c] = e_tmp[pl.ds(c, SUBS, stride=cols), :]

    def up(part, sender, target):
        return pltpu.make_async_remote_copy(
            src_ref=e_ref.at[part], dst_ref=e_all.at[sender, part], send_sem=e_send.at[target],
            recv_sem=e_recv.at[(part.start + part.size) // blocks, sender], device_id=(p, target), device_id_type=MESH)

    def down(part, sender, target):
        return pltpu.make_async_remote_copy(
            src_ref=e_ref.at[part, pl.ds(0, cols - 1)], dst_ref=e_all.at[sender, part, pl.ds(0, cols - 1)],
            send_sem=e_send.at[target], recv_sem=e_recv.at[(part.start + part.size) // blocks, sender],
            device_id=(p, target), device_id_type=MESH)

    def when(cond, act):
        @pl.when(cond)
        def _():
            act()

    def b_copy(k, sender, target):
        return pltpu.make_async_remote_copy(
            src_ref=b_ref, dst_ref=b_all.at[sender], send_sem=b_send, recv_sem=b_recv,
            device_id=(target, q), device_id_type=MESH)

    def k_copy(tp, tq):
        return pltpu.make_async_remote_copy(
            src_ref=k_ref.at[0], dst_ref=k_all.at[me], send_sem=k_send, recv_sem=k_recv,
            device_id=(tp, tq), device_id_type=MESH)

    def send_edges(begin, end):
        part = pl.ds(begin, end - begin)
        for k in range(nq):
            far = nq - 1 - k
            when(far > q, lambda: up(part, q, far).start())
            when(k < q, lambda: down(part, q, k).start())

    late = 4 * q >= 3 * nq

    def meet(begin, end):
        pl.semaphore_wait(barrier, total - 1)
        send_edges(begin, end)

    arrive(0)
    block(0)
    for b in range(1, blocks):
        arrive(b)
        block(b)
        side_of(b - 1)
        if b == blocks - 2:
            when(late, lambda: meet(0, b))
    when(jnp.logical_not(late), lambda: meet(0, blocks - 2))

    k0, k1 = iotas(per * cols, LANES)
    corner = jnp.zeros((per * cols, LANES), F32)
    for b in range(blocks):
        edge = jnp.broadcast_to(b_ref[b][:, width - 1:], (per * cols, LANES))
        corner = jnp.where(k1 == b * per * cols + k0, edge, corner)
    k_ref[0] = jnp.sum(corner, axis=0, keepdims=True)
    k_all[pl.ds(me, 1)] = k_ref[...]
    others(lambda tp, tq: k_copy(tp, tq).start())
    send_edges(blocks - 2, blocks - 1)
    side_of(blocks - 1)
    send_edges(blocks - 1, blocks)
    for k in range(1, np_):
        b_copy(k, p, lax.rem(p + k, np_)).start()

    r0, _ = iotas(n, LANES)

    def factors(r, _):
        for i in range(steps):
            row = (r * np_ + p) * tile + (r0 // cols) * steps + i
            rf_ref[r, pl.ds(i * n, n), :] = 1.0 / jnp.sqrt((row + 1).astype(F32))
        return 0

    lax.fori_loop(0, rows_here, factors, 0)

    pltpu.make_async_copy(b_all.at[pl.ds(0, np_ - 1)], b_all.at[pl.ds(0, np_ - 1)], b_recv).wait()
    rows = groups * cols
    s_all = b_ref[...].reshape(rows, width)
    s_lt = jnp.zeros_like(s_all)
    for k in range(np_):
        value = jnp.where(k == p, 0.0, b_all[k].reshape(rows, width))
        s_all = s_all + value
        s_lt = s_lt + jnp.where(k < p, value, 0.0)
    o, s = iotas(rows, rows)
    strict = ((o // (rows_here * cols) == s // (rows_here * cols)) & (lax.rem(o, cols) == lax.rem(s, cols))
              & (s // cols < o // cols)).astype(F32)
    pre = lax.dot_general(strict, s_all, NN, precision=HIGH, preferred_element_type=F32)
    d_ref[...] = (pre + s_lt).reshape(blocks, per * cols, width)

    def sums(b):
        base = jnp.zeros((SUBS, LANES), F32)
        for c in range(cols):
            whole, before = e_ref[b, c], jnp.zeros((SUBS, LANES), F32)
            for k in range(nq):
                value = e_all[k, b, c]
                before = before + jnp.where(k < q, value, 0.0)
                if c < cols - 1:
                    whole = whole + jnp.where(k == q, 0.0, value)
            c_ref[b, pl.ds(c, SUBS, stride=cols), :] = base + before
            base = base + whole

    def collect(begin, end):
        part = pl.ds(begin, end - begin)
        for k in range(nq):
            when(k < q, lambda: up(part, k, k).wait_recv())
            when(k > q, lambda: down(part, k, k).wait_recv())
        for b in range(begin, end):
            sums(b)

    collect(0, blocks - 1)
    pltpu.make_async_copy(k_all.at[pl.ds(0, total - 1)], k_all.at[pl.ds(0, total - 1)], k_send).wait()
    pltpu.make_async_copy(b_all.at[pl.ds(0, np_ - 1)], b_all.at[pl.ds(0, np_ - 1)], b_send).wait()
    for k in range(nq):
        when(k > q, lambda: up(pl.ds(0, blocks), q, k).wait_send())
        when(k < q, lambda: down(pl.ds(0, blocks), q, k).wait_send())
    collect(blocks - 1, blocks)

    pltpu.make_async_copy(k_all.at[pl.ds(0, total - 1)], k_all.at[pl.ds(0, total - 1)], k_recv).wait()
    value = k_all.reshape(total, LANES)[...]
    d0, _ = iotas(total, LANES)
    left = jnp.where(lax.rem(d0, nq) < q, value, 0.0)
    add = lambda v: jnp.sum(v, axis=0, keepdims=True)
    a_all, a_lt = add(left), add(jnp.where(d0 // nq < p, left, 0.0))
    c_all, c_lt = add(value), add(jnp.where(d0 // nq < p, value, 0.0))
    out, src = iotas(rows, LANES)
    out_g, src_g = out // cols, src // cols
    out_c, src_c = lax.rem(out, cols), lax.rem(src, cols)
    same_g = out_g == src_g
    above = (out_g // rows_here == src_g // rows_here) & (src_g < out_g)
    weigh = lambda strict, all_rows, lt_rows: (
        jnp.where(above & strict, all_rows, 0.0) + jnp.where(same_g & strict, lt_rows, 0.0))
    corner = jnp.sum(weigh(src_c == out_c, a_all, a_lt) + weigh(src_c < out_c, c_all, c_lt), axis=1, keepdims=True)
    d_ref[...] = d_ref[...] + corner.reshape(blocks, per * cols, 1)


def finish(np_, nq, rows_here, t_ref, pt_ref, c_ref, d_ref, rf_ref, out_hbm, obuf, cb_refs, sem):
    groups, rows, width = t_ref.shape
    cols = out_hbm.shape[3]
    n = SUBS * cols
    steps = rows // n
    per = LANES // steps
    lanes = width // LANES
    q = lax.axis_index("pcol")
    c0, c1 = iotas(n, width)
    cf = 1.0 / jnp.sqrt(((lax.rem(c0, cols) * nq + q) * width + c1 + 1).astype(F32))
    pitch = (steps + 1) * lanes
    sub, _ = iotas(per * cols, width)

    def copies(g):
        return [pltpu.make_async_copy(obuf.at[g, k, pl.ds(0, steps)], out_hbm.at[g, k // cols, :, k % cols], sem)
                for k in range(n)]

    def turned(g):
        return pltpu.roll(c_ref[g // per], LANES - lax.rem(g, per) * steps, 1)

    def spread(c, i):
        return jnp.broadcast_to(c[:, i:i + 1], (n, LANES))

    first = turned(0)
    for i in range(steps):
        cb_refs[0][pl.ds(i * n, n), :] = spread(first, i)

    def pair(b, ahead):
        for slot in range(2):
            g = b * 2 + slot
            r = lax.rem(g, rows_here)
            d = jnp.where(sub // cols == lax.rem(g, per), d_ref[g // per], 0.0)
            shift = cols
            while shift < per * cols:
                d = d + pltpu.roll(d, shift, 0)
                shift *= 2
            d = pt_ref[g] + jnp.concatenate([d] * (n // (per * cols)), axis=0)
            dst = obuf.at[g].reshape(n * pitch, LANES)
            later = turned(lax.rem(g + 2, groups))
            for i in range(steps):
                cb_refs[1 - slot][pl.ds(i * n, n), :] = spread(ahead, i)
            for i in range(steps):
                cut = pl.ds(i * n, n)
                cb, v, f = cb_refs[slot][cut, :], t_ref[g, cut, :], rf_ref[r, cut, :]
                for t in range(lanes):
                    col = slice(t * LANES, (t + 1) * LANES)
                    o = (v[:, col] + (cb + d[:, col])) * (f * cf[:, col])
                    for h in range(0, n, 8):
                        dst[pl.ds(h * pitch + i * lanes + t, 8, stride=pitch), :] = o[h:h + 8]
            ahead = later
            for copy in copies(g):
                copy.start()
        return ahead

    lax.fori_loop(0, groups // 2, pair, turned(1))

    pltpu.make_async_copy(out_hbm, out_hbm, sem).wait()


def solution(mesh):
    np_, nq = mesh.shape["prow"], mesh.shape["pcol"]

    def shards(matrix):
        batch, rows_here, _, tile, cols, _, width = matrix.shape
        groups, lanes = batch * rows_here, width // LANES
        steps, n, total = tile // SUBS, SUBS * cols, np_ * nq
        per = LANES // steps
        blocks = groups // per
        x = pltpu.with_memory_space_constraint(matrix.reshape(groups, tile, cols, width), pltpu.HBM)
        dma = pltpu.SemaphoreType.DMA
        vmem = pl.BlockSpec(memory_space=pltpu.VMEM)
        carried = pl.pallas_call(
            functools.partial(local, np_, nq, rows_here),
            out_shape=(jax.ShapeDtypeStruct((groups, tile * cols, width), F32),
                       jax.ShapeDtypeStruct((groups, n, width), F32),
                       jax.ShapeDtypeStruct((blocks, n, LANES), F32),
                       jax.ShapeDtypeStruct((blocks, per * cols, width), F32),
                       jax.ShapeDtypeStruct((rows_here, tile * cols, LANES), F32)),
            in_specs=[pl.BlockSpec(memory_space=pltpu.HBM)],
            out_specs=(vmem,) * 5,
            scratch_shapes=[
                pltpu.VMEM((groups, tile, cols, width), BF16),
                pltpu.VMEM((width, width), BF16),
                pltpu.VMEM((n, LANES), F32),
                pltpu.VMEM((blocks, cols, SUBS, LANES), F32),
                pltpu.VMEM((blocks, per * cols, width), F32),
                pltpu.VMEM((1, 1, LANES), F32),
                pltpu.VMEM((nq, blocks, cols, SUBS, LANES), F32),
                pltpu.VMEM((np_, blocks, per * cols, width), F32),
                pltpu.VMEM((total, 1, LANES), F32),
                dma((blocks,)), dma((nq,)), dma((2, nq)), dma, dma, dma, dma,
            ],
            compiler_params=pltpu.CompilerParams(
                collective_id=0, has_side_effects=True, vmem_limit_bytes=24 * 2**20),
            name="local",
        )(x)
        out = pl.pallas_call(
            functools.partial(finish, np_, nq, rows_here),
            out_shape=jax.ShapeDtypeStruct((groups, SUBS, steps, cols, lanes, LANES), F32),
            in_specs=[vmem] * 5,
            out_specs=pl.BlockSpec(memory_space=pl.ANY),
            scratch_shapes=[
                pltpu.VMEM((groups, n, steps + 1, lanes, LANES), F32),
                [pltpu.VMEM((tile * cols, LANES), F32)] * 2,
                dma,
            ],
            compiler_params=pltpu.CompilerParams(vmem_limit_bytes=24 * 2**20),
            name="finish",
        )(*carried)
        return out.reshape(matrix.shape)

    spec = P(None, None, "prow", None, None, "pcol", None)
    return jax.shard_map(shards, mesh=mesh, in_specs=(spec,), out_specs=spec, check_vma=False)
```
